128 devices in a mesh: row: 2 (over x_lo), col: 4 (over y), layer: 16 (over z, x_hi, core).
Axes of the slice: x: 4 (x_hi: 2, x_lo: 2; x = x_hi * 2 + x_lo), y: 4, z: 4, core: 2. Of those that a mesh axis runs over, the one named last changes fastest.
Arguments:
- object_field: float32 [2, 512, 1024], P(None, 'row', 'col'), may hold values from -6 to 6
- probe_modes: float32 [2, 4, 256, 256], replicated, may hold values from -6 to 6
- amplitudes: float32 [128, 256, 256], P(('row', 'col', 'layer')), may hold values from 0 to 4
- offsets: int32 [128, 2], P(('row', 'col', 'layer')), may hold values from 0 to 768, as said below
Outputs:
- new_object: float32 [2, 512, 1024], P(None, 'row', 'col')
The draws below stay inside these ranges and needn't reach their ends.
Inputs may be any that keep to these rules, and one draw needn't show every extreme that they name: `offsets`: every patch lies inside the 512 x 1024 object. A position held by the device at tile (r, c) has its corner inside that tile: rows r * 256 to (r + 1) * 256 - 1 and columns c * 256 to (c + 1) * 256 - 1. On a device whose tile row is not the last, its first position's patch reaches into the next tile row.
All inputs are finite; a program needn't handle non-finite values.
Results may differ from the reference program's by a relative error of at most 0.0001.
Values sent between devices are 32-bit elements; how exact they have to be, the bound alone decides.
No kernel may reach another device: no remote copies, remote signals or barrier semaphores. Data moves between devices by JAX's collectives and lax.ppermute only.
A program may use at most 64 MiB of HBM per device.

```python
import jax
import jax.numpy as jnp
from jax import lax

PATCH = 256
MODES = 4
TILE_R = 256
TILE_C = 256
POS_DEV = 1
OBJ_R = 512
OBJ_C = 1024
POSITIONS = 128
N_ROW = 2
N_COL = 4
N_LAYER = 16


def draw_offsets(key, part):
    index = jnp.arange(POSITIONS, dtype=jnp.int32)
    device = index // POS_DEV
    slot = index % POS_DEV
    tile_row = device // (N_COL * N_LAYER)
    tile_col = device // N_LAYER % N_COL
    key_rows, key_cols = jax.random.split(jax.random.fold_in(key, 17))
    rows_high = jnp.where(tile_row == N_ROW - 1, TILE_R - PATCH + 1, TILE_R)
    rows_low = jnp.where((slot == 0) & (tile_row < N_ROW - 1), TILE_R - PATCH + 1, 0)
    draw_rows = jax.random.randint(key_rows, (POSITIONS,), 0, 1 << 30, dtype=jnp.int32)
    local_rows = rows_low + draw_rows % (rows_high - rows_low)
    cols_high = jnp.where(tile_col == N_COL - 1, TILE_C - PATCH + 1, TILE_C)
    draw_cols = jax.random.randint(key_cols, (POSITIONS,), 0, 1 << 30, dtype=jnp.int32)
    local_cols = draw_cols % cols_high
    return jnp.stack([tile_row * TILE_R + local_rows, tile_col * TILE_C + local_cols], axis=-1).astype(jnp.int32)


def steps_of(stream_key, shape, cuts, low, top_value):
    level = 1.0
    for axis_at, parts in cuts:
        draws = jax.random.uniform(jax.random.fold_in(jax.random.fold_in(stream_key, 6), axis_at), (parts,), jnp.float32, low / len(cuts), top_value / len(cuts))
        level = level * jnp.repeat(jnp.exp(draws), shape[axis_at] // parts).reshape((-1,) + (1,) * (len(shape) - 1 - axis_at))
    return level


def centred(rng, shape, spread, most, shards=(), kind=jnp.bfloat16):
    entries = jax.random.normal(rng, shape, jnp.float32) * spread
    if len(shards) > 0:
        entries = steps_of(rng, shape, shards, -0.22, 0.18) * entries
    return jnp.clip(entries, min=-most, max=most).astype(kind)


def setup_inputs(seed: int = 0) -> dict:
    seeds = jax.random.split(jax.random.key(seed), 5)
    return {
        "object_field": centred(seeds[0], (2, OBJ_R, OBJ_C), 1.0, 6.0, ((1, 2), (2, 4)), jnp.float32),
        "probe_modes": centred(seeds[1], (2, MODES, PATCH, PATCH), 1.0, 6.0, (), jnp.float32),
        "amplitudes": jnp.clip(4.0 * jax.random.uniform(seeds[2], (POSITIONS, PATCH, PATCH), jnp.float32) ** steps_of(seeds[2], (POSITIONS, PATCH, PATCH), ((0, 128),), -0.2, 0.2), 0.0, 4.0),
        "offsets": draw_offsets(jax.random.fold_in(seeds[4], 71), 0),
    }


SOFTEN = 0.05
DAMPING = 0.5

def reference(object_field, probe_modes, amplitudes, offsets):
    probe = lax.complex(probe_modes[0], probe_modes[1])
    power = lax.optimization_barrier(jnp.sum(probe_modes[0] * probe_modes[0] + probe_modes[1] * probe_modes[1], axis=0))
    zero_index = jnp.int32(0)

    def one_position(index, carry):
        numer, denom = carry
        row_at = offsets[index, 0].astype(jnp.int32)
        col_at = offsets[index, 1].astype(jnp.int32)
        patch = lax.dynamic_slice(object_field, (zero_index, row_at, col_at), (2, PATCH, PATCH))
        exit_wave = probe * lax.complex(patch[0], patch[1])[None]
        far = jnp.fft.fft2(exit_wave, norm='ortho')
        intensity = lax.optimization_barrier(jnp.sum(far.real * far.real + far.imag * far.imag, axis=0))
        ratio = amplitudes[index] / (jnp.sqrt(intensity) + SOFTEN)
        revised = jnp.fft.ifft2(far * ratio[None], norm='ortho')
        contrib = lax.optimization_barrier(jnp.sum(jnp.conj(probe) * revised, axis=0))
        block = jnp.stack([contrib.real, contrib.imag])
        old_block = lax.dynamic_slice(numer, (zero_index, row_at, col_at), (2, PATCH, PATCH))
        numer = lax.dynamic_update_slice(numer, old_block + block, (zero_index, row_at, col_at))
        old_power = lax.dynamic_slice(denom, (row_at, col_at), (PATCH, PATCH))
        denom = lax.dynamic_update_slice(denom, old_power + power, (row_at, col_at))
        return (numer, denom)
    numer0 = jnp.zeros(object_field.shape, jnp.float32)
    denom0 = jnp.zeros(object_field.shape[1:], jnp.float32)
    numer, denom = lax.fori_loop(0, POSITIONS, one_position, (numer0, denom0))
    return (numer + DAMPING * object_field) / (denom + DAMPING)[None]
```

```python
import functools
import itertools
import math

import jax
import jax.numpy as jnp
import ml_dtypes
import numpy as np
from jax import lax
from jax.experimental import pallas as pl
from jax.experimental.pallas import tpu as pltpu
from jax.sharding import PartitionSpec as P

SOFTEN = 0.05
DAMPING = 0.5
AXES = ("row", "col", "layer")
N = 256
H = 128
VM = pl.BlockSpec(memory_space=pltpu.VMEM)
SM = pl.BlockSpec(memory_space=pltpu.SMEM)
F32 = jnp.float32
BF16 = jnp.bfloat16


def routes(mesh):
    rows, cols = mesh.shape["row"], mesh.shape["col"]
    places = list(itertools.product(range(rows), range(cols), range(4), range(2), range(2)))

    def number(r, c, z, h, k):
        return (((r * cols + c) * 4 + z) * 2 + h) * 2 + k

    def route(move):
        found = []
        for place in places:
            target = move(*place)
            if 0 <= target[0] < rows and 0 <= target[1] < cols:
                found.append((number(*place), number(*target)))
        return found

    return dict(
        core=route(lambda r, c, z, h, k: (r, c, z, h, 1 - k)),
        xh=route(lambda r, c, z, h, k: (r, c, z, 1 - h, k)),
        left=route(lambda r, c, z, h, k: (r, c - 1, z, h, k)),
        up=route(lambda r, c, z, h, k: (r - 1, c, z, 1 - h, k)),
        upleft=route(lambda r, c, z, h, k: (r - 1, c - 1, z, h, k)),
        right=route(lambda r, c, z, h, k: (r, c + 1, z, h, k)),
        down=route(lambda r, c, z, h, k: (r + 1, c, z, 1 - h, k)),
        downright=route(lambda r, c, z, h, k: (r + 1, c + 1, z, h, k)),
        z1=route(lambda r, c, z, h, k: (r, c, (z + 1) % 4, h, k)),
        z2=route(lambda r, c, z, h, k: (r, c, (z + 2) % 4, h, k)),
        z3=route(lambda r, c, z, h, k: (r, c, (z + 3) % 4, h, k)),
    )


def tables():
    n = np.arange(H)[:, None]
    q = np.arange(H)[None, :]
    made = []
    for odd in (0, 1):
        angle = 2.0 * math.pi * ((n * (2 * q + odd)) % N) / N
        cos, sin = np.cos(angle) / 16.0, np.sin(angle) / 16.0
        made.append(np.block([[cos, -sin], [sin, cos]]))
    out = []
    for full in (made[0], made[1], made[0].T, made[1].T):
        full = full.astype(np.float32)
        hi = full.astype(ml_dtypes.bfloat16)
        lo = (full - hi.astype(np.float32)).astype(ml_dtypes.bfloat16)
        out.append(np.stack([hi, lo]))
    return np.stack(out)


def spread():
    where = np.zeros((N, N), np.float32)
    for k in range(N):
        where[k, k // 2 + H * (k % 2)] = 1.0
    return np.stack([where, where.T]).astype(ml_dtypes.bfloat16)


def halves(x):
    hi = x.astype(BF16)
    return hi, (x - hi.astype(F32)).astype(BF16)


def dot(a, b):
    return jnp.dot(a, b, preferred_element_type=F32)


def place():
    layer = lax.axis_index("layer")
    return layer // 4, layer // 2 % 2, layer % 2


def local_of(pair, rows, cols):
    return pair[0] - rows, pair[1] - cols


def window(at, start, count, shift_cols):
    base = pl.multiple_of(start // 8 * 8, 8)
    x = pltpu.roll(at[pl.ds(base, count + 8), :], (count + 8 - (start - base)) % (count + 8), 0)
    return pltpu.roll(x[:count], shift_cols, 1)


def rolled(ref, at, lead, shift_rows, shift_cols, first, count):
    x = ref[lead]
    at[0:N, :] = x
    at[N : 2 * N, :] = x
    return window(at, (N - shift_rows + first) % N, count, shift_cols)


def prep_kernel(probe, offs, amp, where, pw, ampp, twice):
    a = offs[0, 0] - lax.axis_index("row") * N
    b = offs[0, 1] - lax.axis_index("col") * N
    for part in range(2):
        for m in range(4):
            pw[part, m] = rolled(probe, twice, (part, m), a, b, 0, N)
    x = amp[0]
    total = None
    for _ in range(3):
        piece = x.astype(BF16)
        x = x - piece.astype(F32)
        moved = dot(dot(where[1], piece).astype(BF16), where[0])
        total = moved if total is None else total + moved
    ampp[0] = total[:H]
    ampp[1] = total[H:]


def quadrants(a, b, first, count):
    rows = first + lax.broadcasted_iota(jnp.int32, (count, N), 0)
    cols = lax.broadcasted_iota(jnp.int32, (count, N), 1)
    low, far = rows < a, cols < b
    return [
        jnp.logical_and(jnp.logical_not(low), jnp.logical_not(far)),
        jnp.logical_and(jnp.logical_not(low), far),
        jnp.logical_and(low, jnp.logical_not(far)),
        jnp.logical_and(low, far),
    ]


def den_kernel(probe, o0, o1, o2, o3, den, power, twice):
    base_row = lax.axis_index("row") * N
    base_col = lax.axis_index("col") * N
    z, _, _ = place()
    total = jnp.zeros((N, N), F32)
    for m in range(4):
        total = total + probe[0, m] * probe[0, m] + probe[1, m] * probe[1, m]
    twice[0:N, :] = total
    twice[N : 2 * N, :] = total
    sums = [jnp.zeros((64, N), F32) for _ in range(4)]
    for o in (o0, o1, o2, o3):
        a, b = o[0, 0] - base_row, o[0, 1] - base_col
        x = window(twice, (N - a + 64 * z) % N, 64, b)
        for q, mask in enumerate(quadrants(a, b, 64 * z, 64)):
            sums[q] = sums[q] + jnp.where(mask, x, 0.0)
    for q in range(4):
        den[q] = sums[q]


def wave_kernel(offs, obj, rm, ro, bm, bo, dm, do, pw, amp, tab, own, s1, s2, s3, w, lh, ll, y, acc):
    a = offs[0, 0] - lax.axis_index("row") * N
    b = offs[0, 1] - lax.axis_index("col") * N
    z, _, k = place()

    for at, right, below, diag in ((k * H, rm, bm, dm), ((1 - k) * H, ro, bo, do)):
        at = pl.multiple_of(at, H)
        rows = at + lax.broadcasted_iota(jnp.int32, (H, N), 0)
        cols = lax.broadcasted_iota(jnp.int32, (H, N), 1)
        low, far = rows < a, cols < b
        for part in range(2):
            top = jnp.where(far, right[part], obj[part, pl.ds(at, H), :])
            bottom = jnp.where(far, diag[part], below[part])
            w[part, pl.ds(at, H), :] = jnp.where(low, bottom, top)

    def left3(t, x_hi, x_lo):
        return dot(t[0], x_hi) + dot(t[0], x_lo) + dot(t[1], x_hi)

    def right3(x_hi, x_lo, t):
        return dot(x_hi, t[0]) + dot(x_lo, t[0]) + dot(x_hi, t[1])

    me, mo, met, mot = 0, 1, 2, 3
    C = 64
    for m in range(4):
        for r in range(0, N, C):
            pr, pi = pw[0, m, r : r + C, :], pw[1, m, r : r + C, :]
            wr, wi = w[0, r : r + C, :], w[1, r : r + C, :]
            er, ei = pr * wr - pi * wi, pr * wi + pi * wr
            for side, sign in ((0, 1.0), (1, -1.0)):
                for part, e in ((0, er), (1, ei)):
                    u = e[:, :H] + e[:, H:] if side == 0 else e[:, :H] - e[:, H:]
                    hi, lo = halves(u)
                    lh[m, side, r : r + C, part * H : part * H + H] = hi
                    ll[m, side, r : r + C, part * H : part * H + H] = lo
    for m in range(4):
        res = [right3(lh[m, side], ll[m, side], tab[me + side]) for side in range(2)]
        for side in range(2):
            for part in range(2):
                for half, e in ((0, res[0]), (1, res[1])):
                    top = e[:H, part * H : part * H + H]
                    bot = e[H:, part * H : part * H + H]
                    u = top + bot if side == 0 else top - bot
                    hi, lo = halves(u)
                    lh[m, side, part * H : part * H + H, half * H : half * H + H] = hi
                    ll[m, side, part * H : part * H + H, half * H : half * H + H] = lo
    for m in range(4):
        for side in range(2):
            y[m, side] = left3(tab[met + side], lh[m, side], ll[m, side])
    for side in range(2):
        for r in range(0, H, 32):
            power = jnp.zeros((32, N), F32)
            for m in range(4):
                re, im = y[m, side, r : r + 32, :], y[m, side, H + r : H + r + 32, :]
                power = power + re * re + im * im
            ratio = amp[side, r : r + 32, :] / (jnp.sqrt(power) + SOFTEN)
            for m in range(4):
                for part in range(2):
                    hi, lo = halves(y[m, side, part * H + r : part * H + r + 32, :] * ratio)
                    lh[m, side, part * H + r : part * H + r + 32, :] = hi
                    ll[m, side, part * H + r : part * H + r + 32, :] = lo
    for m in range(4):
        p = left3(tab[me], lh[m, 0], ll[m, 0])
        q = left3(tab[mo], lh[m, 1], ll[m, 1])
        for half, u in ((0, p + q), (1, p - q)):
            hi, lo = halves(u)
            for side in range(2):
                for part in range(2):
                    src = (slice(part * H, part * H + H), slice(side * H, side * H + H))
                    dst = (m, side, slice(half * H, half * H + H), slice(part * H, part * H + H))
                    lh[dst] = hi[src]
                    ll[dst] = lo[src]
    for m in range(4):
        p = right3(lh[m, 0], ll[m, 0], tab[met])
        q = right3(lh[m, 1], ll[m, 1], tab[mot])
        for half, u in ((0, p + q), (1, p - q)):
            at = half * H
            xr, xi = u[:, :H], u[:, H:]
            pr, pi = pw[0, m, :, at : at + H], pw[1, m, :, at : at + H]
            cr, ci = pr * xr + pi * xi, pr * xi - pi * xr
            if m == 0:
                acc[0, :, at : at + H] = cr
                acc[1, :, at : at + H] = ci
            else:
                acc[0, :, at : at + H] += cr
                acc[1, :, at : at + H] += ci
    for n, out in enumerate((own, s1, s2, s3)):
        at = pl.multiple_of((z + n) % 4 * 64, 64)
        out[...] = acc[:, pl.ds(at, 64), :]


def unwrap_kernel(o0, o1, o2, o3, x0, x1, x2, x3, den, mine, other):
    base_row = lax.axis_index("row") * N
    base_col = lax.axis_index("col") * N
    z, _, k = place()
    for out, half in ((mine, k), (other, 1 - k)):
        at = pl.multiple_of(half * 32, 32)
        for q in range(4):
            out[q, 2] = den[q, pl.ds(at, 32), :]
        sums = [[jnp.zeros((32, N), F32) for _ in range(2)] for _ in range(4)]
        for o, x in ((o0, x0), (o1, x1), (o2, x2), (o3, x3)):
            a, b = o[0, 0] - base_row, o[0, 1] - base_col
            for q, mask in enumerate(quadrants(a, b, 64 * z + at, 32)):
                for part in range(2):
                    sums[q][part] = sums[q][part] + jnp.where(mask, x[part, pl.ds(at, 32), :], 0.0)
        for q in range(4):
            for part in range(2):
                out[q, part] = sums[q][part]


def shape(*dims, dtype=F32):
    return jax.ShapeDtypeStruct(dims, dtype)


def body(way, object_field, probe_modes, amplitudes, offsets):
    def send(x, name):
        return lax.ppermute(x, AXES, way[name])

    z, h, k = place()
    half = lax.dynamic_slice_in_dim(object_field, k * H, H, 1)
    rm = send(half, "left")
    dm = send(half, "upleft")
    bm = send(half, "up")
    o1, o2, o3 = (send(offsets, name) for name in ("z1", "z2", "z3"))
    pw, ampp = pl.pallas_call(
        prep_kernel,
        in_specs=[VM, SM, VM, VM],
        out_specs=[VM, VM],
        out_shape=[shape(2, 4, N, N), shape(2, H, N)],
        scratch_shapes=[pltpu.VMEM((2 * N, N), F32)],
        name="prep",
    )(probe_modes, offsets, amplitudes, jnp.asarray(spread()))
    den = pl.pallas_call(
        den_kernel,
        in_specs=[VM, SM, SM, SM, SM],
        out_specs=VM,
        out_shape=shape(4, 64, N),
        scratch_shapes=[pltpu.VMEM((8, 128), F32), pltpu.VMEM((2 * N, N), F32)],
        name="den",
    )(probe_modes, offsets, o1, o2, o3)
    ro, bo, do = (send(x, "core") for x in (rm, bm, dm))
    slab = shape(2, 64, N)
    own, s1, s2, s3 = pl.pallas_call(
        wave_kernel,
        in_specs=[SM] + [VM] * 10,
        out_specs=[VM] * 4,
        out_shape=[slab] * 4,
        scratch_shapes=[
            pltpu.VMEM((2, N, N), F32),
            pltpu.VMEM((4, 2, N, N), BF16),
            pltpu.VMEM((4, 2, N, N), BF16),
            pltpu.VMEM((4, 2, N, N), F32),
            pltpu.VMEM((2, N, N), F32),
        ],
        name="waves",
    )(offsets, object_field, rm, ro, bm, bo, dm, do, pw, ampp, jnp.asarray(tables()))
    x2, x1, x3 = send(s2, "z2"), send(s1, "z1"), send(s3, "z3")
    mine, other = pl.pallas_call(
        unwrap_kernel,
        in_specs=[SM] * 4 + [VM] * 5,
        out_specs=[VM] * 2,
        out_shape=[shape(4, 3, 32, N)] * 2,
        name="unwrap",
    )(offsets, o1, o2, o3, own, x1, x2, x3, den)
    quads = mine + send(other, "core")
    share = quads[0]
    share = share + send(quads[1], "right") + send(quads[2], "down") + send(quads[3], "downright")
    share = share + send(share, "xh")
    own_part = lax.dynamic_slice_in_dim(object_field, z * 64 + k * 32, 32, 1)
    updated = (share[:2] + DAMPING * own_part) / (share[2] + DAMPING)[None]
    around = [updated, *(send(updated, name) for name in ("z1", "z2", "z3"))]
    mixed = jnp.stack(around, axis=1)
    swapped = send(mixed, "core")
    both = jnp.stack([mixed, swapped], axis=2)
    both = jnp.where(k == 0, both, both[:, :, ::-1])
    order = (z - jnp.arange(4)) % 4
    both = both[:, order]
    return both.reshape(2, N, N)


def solution(mesh):
    placed = (
        P(None, "row", "col"),
        P(),
        P(("row", "col", "layer"), None, None),
        P(("row", "col", "layer"), None),
    )
    return jax.shard_map(
        functools.partial(body, routes(mesh)),
        mesh=mesh,
        in_specs=placed,
        out_specs=P(None, "row", "col"),
        check_vma=False,
    )
```
